32 devices in a mesh: lag: 2 (over core), space: 16 (over z, y, x).
Axes of the slice: x: 2, y: 2, z: 4, core: 2. Of those that a mesh axis runs over, the one named last changes fastest.
Arguments:
- ensemble: bfloat16 [2, 64, 65536], P('lag', None, 'space'), may hold values from -6 to 6
- obs_pert: bfloat16 [2, 64, 16384], P('lag', None, 'space'), may hold values from -6 to 6
- obs_innov: bfloat16 [2, 16384], P('lag', 'space'), may hold values from -12 to 12
- obs_rinv: bfloat16 [2, 16384], P('lag', 'space'), may hold values from 0.019897461 to 0.5
- obs_tile: int32 [2, 16384, 1], P('lag', 'space'), may hold values from 0 to 15; in each aligned block of 1024 rows (0 to 1023, 1024 to 2047, ..., all dimensions but the last counted through in order) at most 128 rows name the same one
- obs_column: int32 [2, 16384], P('lag', 'space'), may hold values from 0 to 4095
- obs_count: int32 [2, 16], P('lag', 'space'), may hold values from 512 to 1024, as said below
Outputs:
- analysis: bfloat16 [2, 64, 65536], P('lag', None, 'space')
The draws below stay inside these ranges and needn't reach their ends.
Inputs may be any that keep to these rules, and one draw needn't show every extreme that they name: `obs_tile`: among the 1024 slots of one device at one lag, no tile is named more than 128 times. `obs_count`: slots of a device past its count are not used; in every draw some device uses all 1024.
All inputs are finite; a program needn't handle non-finite values.
Results may differ from the reference program's by a relative error of at most 0.0022.
The reference program's roundings to bfloat16 on the way count: a program that leaves them out, or rounds other values in their place, can miss the bound.
Values may be sent and summed in bfloat16 or wider, within the bound.
A program may use at most 64 MiB of HBM per device.

```python
import math
import jax
import jax.numpy as jnp
import numpy as np
from jax import lax

MEMBERS = 64
COLS_DEV = 4096
SPACING = 512
OBS_DEV = 1024
NS_ITERS = 6
TILES = 16
LAGS = 2
NCOLS = 65536
OBS = 16384
PTS = 8
NPTS = 128
RADIUS = 2048
SLOT = 128
RECV = 2048


def draw_obs_count(key, part):
    base = jax.random.randint(jax.random.fold_in(key, 11), (LAGS, TILES), OBS_DEV // 2, OBS_DEV + 1)
    chosen = jax.random.randint(jax.random.fold_in(key, 12), (), 0, LAGS * TILES)
    flat = base.reshape(-1)
    flat = jnp.where(jnp.arange(LAGS * TILES) == chosen, OBS_DEV, flat)
    return flat.reshape(LAGS, TILES).astype(jnp.int32)


def touch_ends(values, own_key, least, top_value):
    longest = values.shape.index(max(values.shape))
    spots = []
    for shift in (0, 1):
        where = [jax.random.randint(jax.random.fold_in(own_key, axis), (), 0, length) for axis, length in enumerate(values.shape)]
        where[longest] = (where[longest] + shift) % values.shape[longest]
        spots.append(tuple(where))
    return values.at[spots[0]].set(least).at[spots[1]].set(top_value)


def steps_of(key, extent, shards, least, top_value):
    level = 1.0
    for position, blocks in shards:
        draws = jax.random.uniform(jax.random.fold_in(jax.random.fold_in(key, 6), position), (blocks,), jnp.float32, least / len(shards), top_value / len(shards))
        level = level * jnp.repeat(jnp.exp(draws), extent[position] // blocks).reshape((-1,) + (1,) * (len(extent) - 1 - position))
    return level


def shared_out(key, own, number, rows, amount, top, reach, lean):
    ranking = jax.random.permutation(key, amount)
    heavy_load, ordinary = shares(amount, rows * top, reach, lean, True), shares(amount, rows * top, reach, lean, False)
    places = jnp.arange(amount)

    def named(sizes, rotation):
        used = int((sizes > 0).sum())
        fixed = max(1, used // 4)
        passed = fixed + (places - fixed + rotation * (used - fixed)) % max(1, amount - fixed)
        return jnp.zeros((amount,), jnp.int32).at[ranking[jnp.where(places < fixed, places, passed)]].set(jnp.asarray(sizes, jnp.int32))

    sizes = jnp.where(number % 4 == 0, named(heavy_load, number // 4), named(ordinary, number - number // 4 - 1))
    mixed = jax.random.permutation(jax.random.fold_in(own, 3), amount)
    source_of, receiver = mixed[0:amount // 2 * 2:2], mixed[1:amount // 2 * 2:2]
    room = jnp.minimum(sizes[source_of] - 1, reach - sizes[receiver]) // 2
    room = jnp.where((source_of == ranking[0]) | (receiver == ranking[0]) | (sizes[receiver] == 0), 0, jnp.maximum(room, 0))
    passed = jax.random.randint(jax.random.fold_in(own, 4), (amount // 2,), 0, 1 << 20) % (room + 1)
    sizes = sizes.at[source_of].add(-passed).at[receiver].add(passed)
    items = jnp.searchsorted(jnp.cumsum(sizes), jnp.arange(rows * top), side="right").astype(jnp.int32)
    table = items.reshape(top, rows).T
    table = table[jax.random.permutation(jax.random.fold_in(own, 1), rows)]
    rotation = jax.random.randint(jax.random.fold_in(own, 2), (rows, 1), 0, top)
    return jnp.take_along_axis(table, (jnp.arange(top)[None, :] + rotation) % top, axis=1)


def shares(number_of, total, reach, skew, full):
    portions = [(1 << 20) // math.isqrt(rank ** skew) + 1 for rank in range(1, number_of + 1)]
    largest = reach if full else min(reach, max(-(-total // number_of), total * portions[0] // sum(portions)))
    least = 1 if total - largest >= number_of - 1 else 0
    given, rest = [largest] + [least] * (number_of - 1), total - largest - least * (number_of - 1)
    while rest > 0:
        movable = [i for i in range(1, number_of) if given[i] < largest] or [i for i in range(1, number_of) if given[i] < reach]
        pool, remaining = sum([portions[i] for i in movable]), rest
        for i in movable:
            more = min(reach - given[i], max(1, remaining * portions[i] // pool), rest)
            given[i] = given[i] + more
            rest = rest - more
    return np.array(given)


def centred(own_key, dims, width, limit, split=(), kind=jnp.bfloat16):
    result = jax.random.normal(own_key, dims, jnp.float32) * width
    if len(split) > 0:
        result = steps_of(own_key, dims, split, -0.22, 0.18) * result
    return jnp.clip(result, min=-limit, max=limit).astype(kind)


def setup_inputs(seed: int = 0) -> dict:
    key_of = jax.random.split(jax.random.key(seed), 8)
    ensemble = centred(key_of[0], (LAGS, MEMBERS, NCOLS), 1.0, 6.0, ((0, 2), (2, 16)))
    obs_pert = centred(key_of[1], (LAGS, MEMBERS, OBS), 1.0, 6.0, ((0, 2), (2, 16)))
    obs_innov = centred(key_of[2], (LAGS, OBS), 2.0, 12.0, ((0, 2), (1, 16)))
    obs_rinv = jnp.clip(jnp.exp(math.log(0.5) - 3.224016 * jax.random.uniform(key_of[3], (LAGS, OBS), jnp.float32) ** steps_of(key_of[3], (LAGS, OBS), ((0, 2), (1, 16)), -0.2, 0.2)), 0.019897461, 0.5).astype(jnp.bfloat16)
    obs_tile_keys = jax.random.split(jax.random.fold_in(key_of[4], 1), LAGS * OBS // OBS_DEV)
    obs_tile_turns = jax.random.permutation(jax.random.fold_in(key_of[4], 3), LAGS * OBS // OBS_DEV)
    obs_tile = jax.vmap(lambda own, number: shared_out(jax.random.fold_in(key_of[4], 2), own, number, OBS_DEV, TILES, 1, SLOT, 1))(obs_tile_keys, obs_tile_turns).reshape((LAGS, OBS, 1))
    obs_column = touch_ends(jax.random.randint(key_of[5], (LAGS, OBS), 0, COLS_DEV), jax.random.fold_in(key_of[5], 1), 0, COLS_DEV - 1).astype(jnp.int32)
    obs_count = draw_obs_count(jax.random.fold_in(key_of[7], 71), 0)
    return {"ensemble": ensemble, "obs_pert": obs_pert, "obs_innov": obs_innov, "obs_rinv": obs_rinv, "obs_tile": obs_tile, "obs_column": obs_column, "obs_count": obs_count}


def point_moments(centers, pert, weight, innov, places, radius):
    distance = jnp.abs(places[None, :] - centers[:, None])
    tapers = jnp.square(jnp.maximum(1.0 - distance / radius, 0.0)) * weight[None, :]
    scaled = (pert.astype(jnp.float32)[None] * tapers[:, None, :]).astype(jnp.bfloat16)
    gram_mats = jnp.einsum('gko,jo->gkj', scaled.astype(jnp.float32), pert.astype(jnp.float32))
    drive_vec = jnp.einsum('gko,o->gk', scaled.astype(jnp.float32), innov.astype(jnp.float32))
    return (gram_mats, drive_vec)

def chain_product(left_mats, right_mats):
    return jnp.einsum('pij,pjk->pik', left_mats, right_mats, precision=lax.Precision.HIGHEST)

def transform(gram_mats, drive_vec):
    identity = jnp.eye(MEMBERS, dtype=jnp.float32)
    gram_mats = gram_mats + (MEMBERS - 1.0) * identity
    norm_scale = jnp.sqrt(lax.optimization_barrier(jnp.sum(gram_mats * gram_mats, axis=(1, 2))))
    upper_iter = gram_mats / norm_scale[:, None, None]
    lower_iter = jnp.broadcast_to(identity, gram_mats.shape)
    for sweep in range(NS_ITERS):
        middle = 1.5 * identity - 0.5 * chain_product(lower_iter, upper_iter)
        upper_iter = chain_product(upper_iter, middle)
        lower_iter = chain_product(middle, lower_iter)
    inv_root = lower_iter / jnp.sqrt(norm_scale)[:, None, None]
    inner = jnp.einsum('pij,pj->pi', inv_root, drive_vec, precision=lax.Precision.HIGHEST)
    mean_shift = jnp.einsum('pij,pj->pi', inv_root, inner, precision=lax.Precision.HIGHEST)
    full_weights = math.sqrt(MEMBERS - 1.0) * inv_root + mean_shift[:, :, None]
    return full_weights - lax.optimization_barrier(jnp.mean(full_weights, axis=1, keepdims=True)) + 1.0 / MEMBERS

def reference(ensemble, obs_pert, obs_innov, obs_rinv, obs_tile, obs_column, obs_count):
    centers = (jnp.arange(PTS).astype(jnp.int32) * SPACING + SPACING // 2).astype(jnp.float32)
    offsets = jnp.repeat(jnp.array([-COLS_DEV, 0, COLS_DEV], dtype=jnp.int32), RECV)

    def lag_weights(inputs):
        pert, innov, rinv, tile, column, count = inputs
        slot_ids = jnp.arange(OBS).astype(jnp.int32)
        source = slot_ids // OBS_DEV
        is_valid = slot_ids % OBS_DEV < count[source]
        destination = tile[:, 0]
        dest_hits = (destination[:, None] == jnp.arange(TILES).astype(jnp.int32)[None, :]).astype(jnp.int32)
        dest_hits = dest_hits.reshape(TILES, OBS_DEV, TILES)
        before = jnp.cumsum(dest_hits, axis=1) - dest_hits
        rank = lax.optimization_barrier(jnp.sum(before * dest_hits, axis=2)).reshape(-1)
        placed = destination * RECV + source * SLOT + rank
        weight = jnp.where(is_valid, rinv, jnp.zeros_like(rinv))
        bucket_pert = jnp.zeros((MEMBERS, TILES * RECV), jnp.bfloat16).at[:, placed].set(pert)
        bucket_meta = jnp.zeros((2, TILES * RECV), jnp.bfloat16).at[:, placed].set(jnp.stack([weight, innov]))
        bucket_cols = jnp.zeros((TILES * RECV,), jnp.int32).at[placed].set(column)
        bucket_pert = bucket_pert.reshape(MEMBERS, TILES, RECV)
        bucket_meta = bucket_meta.reshape(2, TILES, RECV)
        bucket_cols = bucket_cols.reshape(TILES, RECV)

        def tile_weights(tile_index):
            chosen = (tile_index + jnp.arange(-1, 2).astype(jnp.int32)) % TILES
            window_pert = jnp.take(bucket_pert, chosen, axis=1).reshape(MEMBERS, 3 * RECV)
            window_meta = jnp.take(bucket_meta, chosen, axis=1).reshape(2, 3 * RECV)
            window_cols = jnp.take(bucket_cols, chosen, axis=0).reshape(-1)
            places = (window_cols + offsets).astype(jnp.float32)
            gram_mats, drive_vec = point_moments(centers, window_pert, window_meta[0].astype(jnp.float32), window_meta[1], places, RADIUS)
            return transform(gram_mats, drive_vec)
        per_tile = lax.map(tile_weights, jnp.arange(TILES).astype(jnp.int32))
        return per_tile.reshape(NPTS, MEMBERS, MEMBERS)
    weights = lax.map(lag_weights, (obs_pert, obs_innov, obs_rinv, obs_tile, obs_column, obs_count))
    identity = jnp.broadcast_to(jnp.eye(MEMBERS, dtype=jnp.float32), (NPTS, MEMBERS, MEMBERS))

    def suffix_step(product, factor):
        newer = chain_product(factor, product)
        return (newer, newer)
    last_carry, products = lax.scan(suffix_step, identity, weights, reverse=True)
    half_span = SPACING // 2
    offsets_in = jnp.arange(SPACING).astype(jnp.float32)
    weight_mid = 1.0 - jnp.abs(offsets_in - half_span) / SPACING
    weight_prev = 1.0 - (offsets_in[:half_span] + half_span) / SPACING
    weight_next = 1.0 - (SPACING + half_span - offsets_in[half_span:]) / SPACING

    def lag_apply(inputs):
        members_block, lag_products = inputs
        rounded = lag_products.astype(jnp.bfloat16).astype(jnp.float32)
        previous = jnp.roll(rounded, 1, axis=0)
        following = jnp.roll(rounded, -1, axis=0)
        blocks = members_block.astype(jnp.float32).reshape(MEMBERS, NPTS, SPACING)
        middle_part = jnp.einsum('jkm,kjo->mjo', rounded, blocks)
        lower_part = jnp.einsum('jkm,kjo->mjo', previous, blocks[:, :, :half_span])
        upper_part = jnp.einsum('jkm,kjo->mjo', following, blocks[:, :, half_span:])
        sides = jnp.concatenate([lower_part * weight_prev, upper_part * weight_next], axis=2)
        analysed = middle_part * weight_mid + sides
        return analysed.reshape(MEMBERS, NCOLS).astype(jnp.bfloat16)
    return lax.map(lag_apply, (ensemble, products))
```

```python
import functools
import math

import jax
import jax.numpy as jnp
from jax import lax
from jax.experimental import pallas as pl
from jax.experimental.pallas import tpu as pltpu
from jax.sharding import PartitionSpec as P

SPACING = 512
NS_ITERS = 6
LANES = 128
META = 16
BASE = 64
F32 = jnp.float32
BF16 = jnp.bfloat16
NT = (((1,), (1,)), ((), ()))


def halves(x):
    hi = x.astype(BF16)
    return hi, (x - hi.astype(F32)).astype(BF16)


def stationary(hi, lo):
    row = jnp.concatenate([hi, lo], axis=1)
    return jnp.concatenate([row, row], axis=0)


def times(left, weights):
    width = weights.shape[1] // 2
    hi, lo = halves(left)
    out = jnp.dot(jnp.concatenate([hi, lo], axis=1), weights, preferred_element_type=F32)
    return out[:, :width] + out[:, width:]


def weights_kernel(
    tiles, lags, slots, group, columns,
    pert_ref, innov_ref, rinv_ref, tile_ref, col_ref, count_ref,
    out_ref,
    msg, snd, rcv, acc, to_left, to_right, from_left, from_right, mine, theirs,
    a2a_send, a2a_recv, halo_send, halo_recv, lag_send, lag_recv,
):
    members, own = pert_ref.shape
    points = columns // SPACING
    half = points // 2
    radius = columns // 2
    pair = 2 * members
    me = lax.axis_index("space")
    my_lag = lax.axis_index("lag")

    barrier = pltpu.get_barrier_semaphore()
    for step in range(1, tiles):
        pl.semaphore_signal(barrier, inc=1, device_id={"space": lax.rem(me + step, tiles)})
    for step in range(1, lags):
        pl.semaphore_signal(barrier, inc=1, device_id={"lag": lax.rem(my_lag + step, lags)})

    slot_id = lax.broadcasted_iota(jnp.int32, (1, own), 1)
    weight = jnp.where(slot_id < count_ref[0, 0], rinv_ref[...].astype(F32), 0.0)
    column = col_ref[...]
    col_hi = (column // BASE).astype(F32)
    col_lo = (column % BASE).astype(F32)
    row = lax.broadcasted_iota(jnp.int32, (META, own), 0)
    meta = jnp.where(row == 0, weight, 0.0)
    meta = jnp.where(row == 1, innov_ref[...].astype(F32), meta)
    meta = jnp.where(row == 2, col_hi, meta)
    meta = jnp.where(row == 3, col_lo, meta)
    msg[0:members, :] = pert_ref[...]
    msg[members:, :] = meta.astype(BF16)

    target = tile_ref[...]
    hits = jnp.where(target == lax.broadcasted_iota(jnp.int32, (tiles, own), 0), 1.0, 0.0)
    tri = jnp.where(
        lax.broadcasted_iota(jnp.int32, (LANES, LANES), 0)
        < lax.broadcasted_iota(jnp.int32, (LANES, LANES), 1),
        1.0, 0.0,
    ).astype(BF16)
    seen = jnp.zeros((tiles, 1), F32)
    ranks = []
    for b in range(own // LANES):
        block = hits[:, b * LANES : (b + 1) * LANES]
        ahead = jnp.dot(block.astype(BF16), tri, preferred_element_type=F32) + seen
        ranks.append(jnp.sum(ahead * block, axis=0, keepdims=True))
        seen = seen + jnp.sum(block, axis=1, keepdims=True)
    rank = jnp.concatenate(ranks, axis=1).astype(jnp.int32)
    key = target * slots + rank
    place = lax.broadcasted_iota(jnp.int32, (slots, own), 0)
    message = msg[...]

    def bucket(dest):
        chosen = jnp.where(place == key - dest * slots, 1.0, 0.0).astype(BF16)
        return lax.dot_general(message, chosen, NT, preferred_element_type=F32).astype(BF16)

    def a2a(step):
        return pltpu.make_async_remote_copy(
            src_ref=snd.at[step], dst_ref=rcv.at[step],
            send_sem=a2a_send.at[step], recv_sem=a2a_recv.at[step],
            device_id={"space": lax.rem(me + step, tiles)},
        )

    for step in range(1, tiles):
        snd[step] = bucket(lax.rem(me + step, tiles))
        if step == 1:
            pl.semaphore_wait(barrier, tiles - 1 + lags - 1)
        else:
            a2a(step - 1).start()
    rcv[0] = bucket(me)
    a2a(tiles - 1).start()

    for first in range(0, tiles, group):
        for step in range(max(first, 1), first + group):
            a2a(step).wait_recv()
        obs = jnp.concatenate([rcv[step] for step in range(first, first + group)], axis=1)
        pert = obs[0:members].astype(F32)
        info = obs[members:].astype(F32)
        obs_weight = info[0:1]
        places = info[2:3] * BASE + info[3:4]
        for k in range(points + 2 * half):
            center = float((k - half) * SPACING + SPACING // 2)
            taper = jnp.maximum(1.0 - jnp.abs(places - center) / radius, 0.0)
            rho = taper * taper * obs_weight
            scaled = (pert * rho).astype(BF16)
            part = lax.dot_general(scaled, obs, NT, preferred_element_type=F32)
            if first == 0:
                acc[k] = part
            else:
                acc[k] += part

    lane = lax.broadcasted_iota(jnp.int32, (members, pair), 1)
    low = lane < members

    def joined(a, b):
        return jnp.concatenate([acc[a, :, 0:members], acc[b, :, 0:members]], axis=1)

    def drive_of(a):
        return acc[a, :, members + 1 : members + 2]

    pairs_side = (half + 2) // 2
    last = points + 2 * half - 1
    left_own = jnp.concatenate([jnp.zeros((members, members), F32), acc[0, :, 0:members]], axis=1)
    for j in range(half + 1):
        left_own = jnp.where(lane == j, drive_of(j), left_own)
    to_left[0] = left_own
    for i in range(1, pairs_side):
        to_left[i] = joined(2 * i - 1, 2 * i)
    right_own = jnp.concatenate([acc[last, :, 0:members], jnp.zeros((members, members), F32)], axis=1)
    for j in range(half + 1):
        right_own = jnp.where(lane == members + j, drive_of(last - half + j), right_own)
    to_right[pairs_side - 1] = right_own
    for i in range(pairs_side - 1):
        to_right[i] = joined(last - half + 2 * i, last - half + 2 * i + 1)

    eye = jnp.where(
        lax.rem(lane, members) == lax.broadcasted_iota(jnp.int32, (members, pair), 0), 1.0, 0.0
    )
    mask_low = jnp.where(low, 1.0, 0.0).astype(BF16)
    mask_high = jnp.where(low, 0.0, 1.0).astype(BF16)

    def diagonal(x):
        return jnp.concatenate([x * mask_low, x * mask_high], axis=0)

    def blocks(x):
        hi, lo = halves(x)
        return stationary(diagonal(hi), diagonal(lo))

    left_copy = pltpu.make_async_remote_copy(
        src_ref=to_left, dst_ref=from_right, send_sem=halo_send.at[0], recv_sem=halo_recv.at[0],
        device_id={"space": lax.rem(me + tiles - 1, tiles)},
    )
    right_copy = pltpu.make_async_remote_copy(
        src_ref=to_right, dst_ref=from_left, send_sem=halo_send.at[1], recv_sem=halo_recv.at[1],
        device_id={"space": lax.rem(me + 1, tiles)},
    )
    left_copy.start()
    right_copy.start()

    count = (points + 2) // 2
    own_pairs = [joined(half - 1 + 2 * i, half + 2 * i) for i in range(count)]
    own_drives = [drive_of(half - 1 + j) for j in range(points + 2)]
    left_copy.wait_recv()
    right_copy.wait_recv()
    lefts = [from_left[i] for i in range(pairs_side)]
    rights = [from_right[i] for i in range(pairs_side)]

    grams, drives = [], []
    for i in range(count):
        total = own_pairs[i] + (members - 1.0) * eye
        if i < pairs_side - 1:
            total = total + lefts[i]
        elif i == pairs_side - 1:
            total = total + jnp.where(low, lefts[i], rights[0])
        else:
            total = total + rights[i - pairs_side + 1]
        grams.append(total)
    for j in range(points + 2):
        if j <= half:
            other = lefts[pairs_side - 1][:, members + j : members + j + 1]
        else:
            other = rights[0][:, j - half - 1 : j - half]
        drives.append(own_drives[j] + other)

    uppers, lowers, scales = [], [], []
    for total in grams:
        squares = jnp.sum(total * total, axis=0, keepdims=True)
        row_low = lax.broadcasted_iota(jnp.int32, (1, pair), 1) < members
        sum_low = jnp.sum(jnp.where(row_low, squares, 0.0), axis=1, keepdims=True)
        sum_high = jnp.sum(jnp.where(row_low, 0.0, squares), axis=1, keepdims=True)
        scale = jnp.sqrt(jnp.where(row_low, sum_low, sum_high))
        scales.append(scale)
        uppers.append(total / scale)

    for sweep in range(NS_ITERS):
        if sweep == 0:
            middles = [1.5 * eye - 0.5 * up for up in uppers]
            lowers = middles
            uppers = [times(up, blocks(mid)) for up, mid in zip(uppers, middles)]
        else:
            middles = [
                1.5 * eye - 0.5 * times(lo, blocks(up)) for lo, up in zip(lowers, uppers)
            ]
            if sweep < NS_ITERS - 1:
                both = [
                    times(jnp.concatenate([up, lo], axis=0), blocks(mid))
                    for up, lo, mid in zip(uppers, lowers, middles)
                ]
                uppers = [x[0:members] for x in both]
                lowers = [x[members:] for x in both]
            else:
                lowers = [times(lo, blocks(mid)) for lo, mid in zip(lowers, middles)]

    results = []
    for i in range(count):
        root = lowers[i] / jnp.sqrt(scales[i])
        top = jnp.where(low, drives[2 * i], 0.0)
        bottom = jnp.where(low, 0.0, drives[2 * i + 1])
        hi, lo = halves(jnp.concatenate([top, bottom], axis=0))
        inner = times(root, stationary(hi, lo))
        shift = times(root, blocks(inner))
        full = math.sqrt(members - 1.0) * root + shift
        results.append(full - jnp.mean(full, axis=0, keepdims=True) + 1.0 / members)
    for i in range(count):
        mine[i] = results[i]

    def lag_copy(step):
        return pltpu.make_async_remote_copy(
            src_ref=mine, dst_ref=theirs.at[step - 1],
            send_sem=lag_send.at[step - 1], recv_sem=lag_recv.at[step - 1],
            device_id={"lag": lax.rem(my_lag + lags - step, lags)},
        )

    for step in range(1, lags):
        lag_copy(step).start()
    for step in range(1, lags):
        lag_copy(step).wait_recv()
        later = my_lag + step < lags
        for i in range(count):
            longer = times(results[i], blocks(theirs[step - 1, i]))
            results[i] = jnp.where(later, longer, results[i])
    for i in range(count):
        out_ref[i] = results[i].astype(BF16)

    for step in range(1, tiles):
        a2a(step).wait_send()
    left_copy.wait_send()
    right_copy.wait_send()
    for step in range(1, lags):
        lag_copy(step).wait_send()


def apply_kernel(members, columns, weights_ref, ens_ref, out_ref):
    points = columns // SPACING
    turned = jnp.concatenate(
        [weights_ref[i].astype(F32).T.astype(BF16) for i in range((points + 2) // 2)], axis=0
    )
    half_span = SPACING // 2
    for s in range(points + 1):
        start = max(s * SPACING - half_span, 0)
        stop = min(s * SPACING + half_span, columns)
        both = jnp.dot(
            turned[s * members : (s + 2) * members], ens_ref[:, start:stop],
            preferred_element_type=F32,
        )
        along = lax.broadcasted_iota(jnp.int32, (1, stop - start), 1).astype(F32)
        second = (along + float(start - (s * SPACING - half_span))) / SPACING
        mixed = both[0:members] * (1.0 - second) + both[members:] * second
        out_ref[:, start:stop] = mixed.astype(BF16)


def per_device(ensemble, obs_pert, obs_innov, obs_rinv, obs_tile, obs_column, obs_count):
    members, columns = ensemble.shape[1:]
    own = obs_pert.shape[2]
    tiles, lags = lax.axis_size("space"), lax.axis_size("lag")
    slot_size = max(2, 2 * own // tiles)
    slots = -(-slot_size // LANES) * LANES
    group = 4
    points = columns // SPACING
    half = points // 2
    count = (points + 2) // 2
    pair = 2 * members
    rows = members + META
    side = ((half + 2) // 2, members, pair)
    vmem = pl.BlockSpec(memory_space=pltpu.VMEM)
    products = pl.pallas_call(
        functools.partial(weights_kernel, tiles, lags, slots, group, columns),
        out_shape=jax.ShapeDtypeStruct((count, members, pair), BF16),
        in_specs=[vmem] * 5 + [pl.BlockSpec(memory_space=pltpu.SMEM)],
        out_specs=vmem,
        scratch_shapes=[
            pltpu.VMEM((rows, own), BF16),
            pltpu.VMEM((tiles, rows, slots), BF16),
            pltpu.VMEM((tiles, rows, slots), BF16),
            pltpu.VMEM((points + 2 * half, members, rows), F32),
            pltpu.VMEM(side, F32),
            pltpu.VMEM(side, F32),
            pltpu.VMEM(side, F32),
            pltpu.VMEM(side, F32),
            pltpu.VMEM((count, members, pair), F32),
            pltpu.VMEM((max(lags - 1, 1), count, members, pair), F32),
            pltpu.SemaphoreType.DMA((tiles,)),
            pltpu.SemaphoreType.DMA((tiles,)),
            pltpu.SemaphoreType.DMA((2,)),
            pltpu.SemaphoreType.DMA((2,)),
            pltpu.SemaphoreType.DMA((max(lags - 1, 1),)),
            pltpu.SemaphoreType.DMA((max(lags - 1, 1),)),
        ],
        compiler_params=pltpu.CompilerParams(collective_id=0, has_side_effects=True),
        name="ensemble_weights",
    )(obs_pert[0], obs_innov, obs_rinv, obs_tile[:, :, 0], obs_column, obs_count)
    analysis = pl.pallas_call(
        functools.partial(apply_kernel, members, columns),
        out_shape=jax.ShapeDtypeStruct((members, columns), BF16),
        in_specs=[vmem] * 2,
        out_specs=vmem,
        name="apply_weights",
    )(products, ensemble[0])
    return analysis[None]


def solution(mesh):
    return jax.shard_map(
        per_device,
        mesh=mesh,
        in_specs=(
            P("lag", None, "space"),
            P("lag", None, "space"),
            P("lag", "space"),
            P("lag", "space"),
            P("lag", "space", None),
            P("lag", "space"),
            P("lag", "space"),
        ),
        out_specs=P("lag", None, "space"),
        check_vma=False,
    )
```

```python
import functools
import math

import jax
import jax.numpy as jnp
from jax import lax
from jax.experimental import pallas as pl
from jax.experimental.pallas import tpu as pltpu
from jax.sharding import PartitionSpec as P

SPACING = 512
NS_ITERS = 6
LANES = 128
META = 16
BASE = 64
F32 = jnp.float32
BF16 = jnp.bfloat16
NT = (((1,), (1,)), ((), ()))


def halves(x):
    hi = x.astype(BF16)
    return hi, (x - hi.astype(F32)).astype(BF16)


def stationary(hi, lo):
    row = jnp.concatenate([hi, lo], axis=1)
    return jnp.concatenate([row, row], axis=0)


def times(left, weights):
    width = weights.shape[1] // 2
    hi, lo = halves(left)
    out = jnp.dot(jnp.concatenate([hi, lo], axis=1), weights, preferred_element_type=F32)
    return out[:, :width] + out[:, width:]


def weights_kernel(
    tiles, lags, slots, group, columns,
    pert_hbm, innov_hbm, rinv_hbm, tile_hbm, col_hbm, count_hbm, ens_hbm,
    out_hbm,
    ens, out, move_sem,
    innov_ref, rinv_ref, tile_ref, col_ref, count_ref, load_sem,
    msg, snd, rcv, acc, to_left, to_right, from_left, from_right, mine, theirs,
    a2a_send, a2a_recv, halo_send, halo_recv, lag_send, lag_recv,
):
    members, own = pert_hbm.shape
    points = columns // SPACING
    half = points // 2
    radius = columns // 2
    pair = 2 * members
    sent = members + META // 2
    me = lax.axis_index("space")
    my_lag = lax.axis_index("lag")

    barrier = pltpu.get_barrier_semaphore()
    order = range(tiles - 1, 0, -1)
    for step in order:
        pl.semaphore_signal(barrier, inc=1, device_id={"space": lax.rem(me + step, tiles)})
    for step in range(1, lags):
        pl.semaphore_signal(barrier, inc=1, device_id={"lag": lax.rem(my_lag + step, lags)})

    loads = [
        pltpu.make_async_copy(source, dest, load_sem.at[n])
        for n, (source, dest) in enumerate((
            (tile_hbm, tile_ref),
            (count_hbm, count_ref),
            (rinv_hbm, rinv_ref),
            (innov_hbm, innov_ref),
            (col_hbm, col_ref),
            (pert_hbm, msg.at[0:members]),
        ))
    ]
    for load in loads:
        load.start()
    for load in loads:
        load.wait()

    slot_id = lax.broadcasted_iota(jnp.int32, (1, own), 1)
    weight = jnp.where(slot_id < count_ref[0, 0], rinv_ref[...].astype(F32), 0.0)
    column = col_ref[...]
    col_hi = (column // BASE).astype(F32)
    col_lo = (column % BASE).astype(F32)
    row = lax.broadcasted_iota(jnp.int32, (META, own), 0)
    meta = jnp.where(row == 0, weight, 0.0)
    meta = jnp.where(row == 1, innov_ref[...].astype(F32), meta)
    meta = jnp.where(row == 2, col_hi, meta)
    meta = jnp.where(row == 3, col_lo, meta)
    msg[members:, :] = meta.astype(BF16)

    target = tile_ref[...]
    hits = jnp.where(target == lax.broadcasted_iota(jnp.int32, (tiles, own), 0), 1.0, 0.0)
    tri = jnp.where(
        lax.broadcasted_iota(jnp.int32, (LANES, LANES), 0)
        < lax.broadcasted_iota(jnp.int32, (LANES, LANES), 1),
        1.0, 0.0,
    ).astype(BF16)
    seen = jnp.zeros((tiles, 1), F32)
    ranks = []
    for b in range(own // LANES):
        block = hits[:, b * LANES : (b + 1) * LANES]
        ahead = jnp.dot(block.astype(BF16), tri, preferred_element_type=F32) + seen
        ranks.append(jnp.sum(ahead * block, axis=0, keepdims=True))
        seen = seen + jnp.sum(block, axis=1, keepdims=True)
    rank = jnp.concatenate(ranks, axis=1).astype(jnp.int32)
    key = target * slots + rank
    place = lax.broadcasted_iota(jnp.int32, (slots, own), 0)
    message = msg[...]

    def bucket(dest):
        chosen = jnp.where(place == key - dest * slots, 1.0, 0.0).astype(BF16)
        return lax.dot_general(message, chosen, NT, preferred_element_type=F32).astype(BF16)

    def a2a(step):
        return pltpu.make_async_remote_copy(
            src_ref=snd.at[step, 0:sent], dst_ref=rcv.at[step, 0:sent],
            send_sem=a2a_send.at[step], recv_sem=a2a_recv.at[step],
            device_id={"space": lax.rem(me + step, tiles)},
        )

    for step in order:
        snd[step] = bucket(lax.rem(me + step, tiles))
    rcv[0] = bucket(me)
    for step in order:
        rcv[step, sent:] = jnp.zeros((members + META - sent, slots), BF16)
    pl.semaphore_wait(barrier, tiles - 1 + lags - 1)
    for step in order:
        a2a(step).start()

    ens_load = pltpu.make_async_copy(ens_hbm, ens, move_sem.at[0])
    ens_load.start()
    arrivals = [0] + list(order)
    for first in range(0, tiles, group):
        for step in arrivals[max(first, 1) : first + group]:
            a2a(step).wait_recv()
        obs = jnp.concatenate([rcv[step] for step in arrivals[first : first + group]], axis=1)
        pert = obs[0:members].astype(F32)
        info = obs[members:].astype(F32)
        obs_weight = info[0:1]
        places = info[2:3] * BASE + info[3:4]

        def moments(ks, obs=obs, pert=pert, places=places, obs_weight=obs_weight, first=first):
            for k in ks:
                center = float((k - half) * SPACING + SPACING // 2)
                taper = jnp.maximum(1.0 - jnp.abs(places - center) / radius, 0.0)
                rho = taper * taper * obs_weight
                scaled = (pert * rho).astype(BF16)
                part = lax.dot_general(scaled, obs, NT, preferred_element_type=F32)
                if first == 0:
                    acc[k] = part
                else:
                    acc[k] += part

        if first + group < tiles:
            moments(range(points + 2 * half))

    lane = lax.broadcasted_iota(jnp.int32, (members, pair), 1)
    low = lane < members

    def joined(a, b):
        return jnp.concatenate([acc[a, :, 0:members], acc[b, :, 0:members]], axis=1)

    def drive_of(a):
        return acc[a, :, members + 1 : members + 2]

    left_copy = pltpu.make_async_remote_copy(
        src_ref=to_left, dst_ref=from_right, send_sem=halo_send.at[0], recv_sem=halo_recv.at[0],
        device_id={"space": lax.rem(me + tiles - 1, tiles)},
    )
    right_copy = pltpu.make_async_remote_copy(
        src_ref=to_right, dst_ref=from_left, send_sem=halo_send.at[1], recv_sem=halo_recv.at[1],
        device_id={"space": lax.rem(me + 1, tiles)},
    )

    pairs_side = (half + 2) // 2
    last = points + 2 * half - 1
    moments(range(half + 1))
    left_own = jnp.concatenate([jnp.zeros((members, members), F32), acc[0, :, 0:members]], axis=1)
    for j in range(half + 1):
        left_own = jnp.where(lane == j, drive_of(j), left_own)
    to_left[0] = left_own
    for i in range(1, pairs_side):
        to_left[i] = joined(2 * i - 1, 2 * i)
    moments(range(last - half, last + 1))
    left_copy.start()
    right_own = jnp.concatenate([acc[last, :, 0:members], jnp.zeros((members, members), F32)], axis=1)
    for j in range(half + 1):
        right_own = jnp.where(lane == members + j, drive_of(last - half + j), right_own)
    to_right[pairs_side - 1] = right_own
    for i in range(pairs_side - 1):
        to_right[i] = joined(last - half + 2 * i, last - half + 2 * i + 1)

    moments(range(half + 1, half + 3))
    right_copy.start()
    moments(range(half + 3, last - half))

    eye = jnp.where(
        lax.rem(lane, members) == lax.broadcasted_iota(jnp.int32, (members, pair), 0), 1.0, 0.0
    )
    mask_low = jnp.where(low, 1.0, 0.0).astype(BF16)
    mask_high = jnp.where(low, 0.0, 1.0).astype(BF16)

    def diagonal(x):
        return jnp.concatenate([x * mask_low, x * mask_high], axis=0)

    def blocks(x):
        hi, lo = halves(x)
        return stationary(diagonal(hi), diagonal(lo))


    count = (points + 2) // 2
    own_pairs = [joined(half - 1 + 2 * i, half + 2 * i) for i in range(count)]
    own_drives = [drive_of(half - 1 + j) for j in range(points + 2)]
    left_copy.wait_recv()
    right_copy.wait_recv()
    lefts = [from_left[i] for i in range(pairs_side)]
    rights = [from_right[i] for i in range(pairs_side)]

    grams, drives = [], []
    for i in range(count):
        total = own_pairs[i] + (members - 1.0) * eye
        if i < pairs_side - 1:
            total = total + lefts[i]
        elif i == pairs_side - 1:
            total = total + jnp.where(low, lefts[i], rights[0])
        else:
            total = total + rights[i - pairs_side + 1]
        grams.append(total)
    for j in range(points + 2):
        if j <= half:
            other = lefts[pairs_side - 1][:, members + j : members + j + 1]
        else:
            other = rights[0][:, j - half - 1 : j - half]
        drives.append(own_drives[j] + other)

    uppers, lowers, scales = [], [], []
    for total in grams:
        squares = jnp.sum(total * total, axis=0, keepdims=True)
        row_low = lax.broadcasted_iota(jnp.int32, (1, pair), 1) < members
        sum_low = jnp.sum(jnp.where(row_low, squares, 0.0), axis=1, keepdims=True)
        sum_high = jnp.sum(jnp.where(row_low, 0.0, squares), axis=1, keepdims=True)
        scale = jnp.sqrt(jnp.where(row_low, sum_low, sum_high))
        scales.append(scale)
        uppers.append(total / scale)

    for sweep in range(NS_ITERS):
        if sweep == 0:
            middles = [1.5 * eye - 0.5 * up for up in uppers]
            lowers = middles
            uppers = [times(up, blocks(mid)) for up, mid in zip(uppers, middles)]
        else:
            middles = [
                1.5 * eye - 0.5 * times(lo, blocks(up)) for lo, up in zip(lowers, uppers)
            ]
            if sweep < NS_ITERS - 1:
                both = [
                    times(jnp.concatenate([up, lo], axis=0), blocks(mid))
                    for up, lo, mid in zip(uppers, lowers, middles)
                ]
                uppers = [x[0:members] for x in both]
                lowers = [x[members:] for x in both]
            else:
                lowers = [times(lo, blocks(mid)) for lo, mid in zip(lowers, middles)]

    results = []
    for i in range(count):
        root = lowers[i] / jnp.sqrt(scales[i])
        top = jnp.where(low, drives[2 * i], 0.0)
        bottom = jnp.where(low, 0.0, drives[2 * i + 1])
        hi, lo = halves(jnp.concatenate([top, bottom], axis=0))
        inner = times(root, stationary(hi, lo))
        shift = times(root, blocks(inner))
        full = math.sqrt(members - 1.0) * root + shift
        results.append(full - jnp.mean(full, axis=0, keepdims=True) + 1.0 / members)
    for i in range(count):
        mine[i] = results[i]

    def lag_copy(step):
        return pltpu.make_async_remote_copy(
            src_ref=mine, dst_ref=theirs.at[step - 1],
            send_sem=lag_send.at[step - 1], recv_sem=lag_recv.at[step - 1],
            device_id={"lag": lax.rem(my_lag + lags - step, lags)},
        )

    for step in range(1, lags):
        lag_copy(step).start()
    for step in range(1, lags):
        lag_copy(step).wait_recv()
        later = my_lag + step < lags
        for i in range(count):
            longer = times(results[i], blocks(theirs[step - 1, i]))
            results[i] = jnp.where(later, longer, results[i])
    turned = jnp.concatenate([results[i].T.astype(BF16) for i in range(count)], axis=0)
    ens_load.wait()
    stores = []
    half_span = SPACING // 2
    for s in range(points + 1):
        start = max(s * SPACING - half_span, 0)
        stop = min(s * SPACING + half_span, columns)
        both = jnp.dot(
            turned[s * members : (s + 2) * members], ens[:, start:stop],
            preferred_element_type=F32,
        )
        along = lax.broadcasted_iota(jnp.int32, (1, stop - start), 1).astype(F32)
        second = (along + float(start - (s * SPACING - half_span))) / SPACING
        mixed = both[0:members] * (1.0 - second) + both[members:] * second
        out[:, start:stop] = mixed.astype(BF16)
        if s % 3 == 2:
            first = max((s - 2) * SPACING - half_span, 0)
            store = pltpu.make_async_copy(
                out.at[:, first:stop], out_hbm.at[:, first:stop], move_sem.at[1 + s // 3]
            )
            store.start()
            stores.append(store)
    for store in stores:
        store.wait()

    for step in range(1, tiles):
        a2a(step).wait_send()
    left_copy.wait_send()
    right_copy.wait_send()
    for step in range(1, lags):
        lag_copy(step).wait_send()


def per_device(ensemble, obs_pert, obs_innov, obs_rinv, obs_tile, obs_column, obs_count):
    members, columns = ensemble.shape[1:]
    own = obs_pert.shape[2]
    tiles, lags = lax.axis_size("space"), lax.axis_size("lag")
    slot_size = max(2, 2 * own // tiles)
    slots = -(-slot_size // LANES) * LANES
    group = 4
    points = columns // SPACING
    half = points // 2
    count = (points + 2) // 2
    pair = 2 * members
    rows = members + META
    side = ((half + 2) // 2, members, pair)
    products = pl.pallas_call(
        functools.partial(weights_kernel, tiles, lags, slots, group, columns),
        out_shape=jax.ShapeDtypeStruct((members, columns), BF16),
        in_specs=[pl.BlockSpec(memory_space=pltpu.HBM)] * 7,
        out_specs=pl.BlockSpec(memory_space=pltpu.HBM),
        scratch_shapes=[
            pltpu.VMEM((members, columns), BF16),
            pltpu.VMEM((members, columns), BF16),
            pltpu.SemaphoreType.DMA((1 + (points + 1) // 3,)),
            pltpu.VMEM((1, own), BF16),
            pltpu.VMEM((1, own), BF16),
            pltpu.VMEM((1, own), jnp.int32),
            pltpu.VMEM((1, own), jnp.int32),
            pltpu.SMEM((1, 1), jnp.int32),
            pltpu.SemaphoreType.DMA((6,)),
            pltpu.VMEM((rows, own), BF16),
            pltpu.VMEM((tiles, rows, slots), BF16),
            pltpu.VMEM((tiles, rows, slots), BF16),
            pltpu.VMEM((points + 2 * half, members, rows), F32),
            pltpu.VMEM(side, F32),
            pltpu.VMEM(side, F32),
            pltpu.VMEM(side, F32),
            pltpu.VMEM(side, F32),
            pltpu.VMEM((count, members, pair), F32),
            pltpu.VMEM((max(lags - 1, 1), count, members, pair), F32),
            pltpu.SemaphoreType.DMA((tiles,)),
            pltpu.SemaphoreType.DMA((tiles,)),
            pltpu.SemaphoreType.DMA((2,)),
            pltpu.SemaphoreType.DMA((2,)),
            pltpu.SemaphoreType.DMA((max(lags - 1, 1),)),
            pltpu.SemaphoreType.DMA((max(lags - 1, 1),)),
        ],
        compiler_params=pltpu.CompilerParams(collective_id=0, has_side_effects=True),
        name="ensemble_weights",
    )(obs_pert[0], obs_innov, obs_rinv, obs_tile[:, :, 0], obs_column, obs_count, ensemble[0])
    return products[None]


def solution(mesh):
    return jax.shard_map(
        per_device,
        mesh=mesh,
        in_specs=(
            P("lag", None, "space"),
            P("lag", None, "space"),
            P("lag", "space"),
            P("lag", "space"),
            P("lag", "space", None),
            P("lag", "space"),
            P("lag", "space"),
        ),
        out_specs=P("lag", None, "space"),
        check_vma=False,
    )
```
